1024 devices in a mesh: col: 64 (over y, x, core), grp: 16 (over z).
Axes of the slice: x: 4, y: 8, z: 16, core: 2. Of those that a mesh axis runs over, the one named last changes fastest.
Arguments:
- profiles: float32 [16384, 116], P('col'), may hold values from -6 to 6
- courant: float32 [16384, 58], P('col'), may hold values from -0.7 to 0.7
- owner_map: int32 [16384], replicated, may hold values from 0 to 16383, as said below
- cloud_flags: int32 [16384], P('col'), may hold values 0 or 1
- crm_state: float32 [2, 58, 64, 16384], P(None, None, 'grp', 'col'), may hold values from -6 to 6
Outputs:
- tendency: float32 [16384, 116], P('col')
- crm_final: float32 [2, 58, 64, 16384], P(None, None, 'grp', 'col')
The draws below stay inside these ranges and needn't reach their ends.
Inputs may be any that keep to these rules, and one draw needn't show every extreme that they name: owner_map is a permutation; physics column p lives in span p // 256, element column e in group e // 256; each group hands at most 6 columns to one span, and exactly 6 to some spans, and every span receives exactly 256 columns.
All inputs are finite; a program needn't handle non-finite values. No bound on the sum of `cloud_flags` on one device may be relied on, other than what follows from the above.
Results may differ from the reference program's by a relative error of at most 0.00002.
Values sent between devices are 32-bit elements; how exact they have to be, the bound alone decides.
No kernel may reach another device: no remote copies, remote signals or barrier semaphores. Data moves between devices by JAX's collectives and lax.ppermute only.
A program may use at most 32 MiB of HBM per device.

```python
import jax
import jax.numpy as jnp

NX = 64
NZ = 58
COLS_DEV = 256
STEPS = 8
COLUMNS = 16384


def draw_owner_map(key, part):
    per_block = COLS_DEV
    block_count = COLUMNS // COLS_DEV
    mean_load = per_block // block_count
    excess = min(2, mean_load)
    key_pattern, key_offset, key_dest, key_source = jax.random.split(jax.random.fold_in(key, 17), 4)
    block_ids = jnp.arange(block_count, dtype=jnp.int32)
    pattern = jnp.where(block_ids % 2 == 0, mean_load + excess, mean_load - excess).astype(jnp.int32)
    pattern = pattern[jax.random.permutation(key_pattern, block_count)]
    offset_of = jax.random.permutation(key_offset, block_count).astype(jnp.int32)
    counts = pattern[(block_ids[None, :] - offset_of[:, None]) % block_count]
    block_ends = jnp.cumsum(counts, axis=1)
    block_starts = block_ends - counts
    slot_ids = jnp.arange(per_block, dtype=jnp.int32)
    dest_block = jnp.sum((slot_ids[None, :, None] >= block_ends[:, None, :]).astype(jnp.int32), axis=2)
    within = slot_ids[None, :] - jnp.take_along_axis(block_starts, dest_block, axis=1)
    arrival = jnp.cumsum(counts, axis=0) - counts
    slot_in_dest = jnp.take_along_axis(arrival, dest_block, axis=1) + within
    dest_shuffle = jax.vmap(lambda subkey: jax.random.permutation(subkey, per_block))(jax.random.split(key_dest, block_count)).astype(jnp.int32)
    physical = dest_block * per_block + dest_shuffle[dest_block, slot_in_dest]
    source_shuffle = jax.vmap(lambda subkey: jax.random.permutation(subkey, per_block))(jax.random.split(key_source, block_count)).astype(jnp.int32)
    element = block_ids[:, None] * per_block + source_shuffle
    return jnp.zeros((COLUMNS,), jnp.int32).at[element.reshape(-1)].set(physical.reshape(-1).astype(jnp.int32))


def with_ends(values, stream_key, least, largest):
    longest = values.shape.index(max(values.shape))
    spots = []
    for shift in (0, 1):
        where = [jax.random.randint(jax.random.fold_in(stream_key, axis), (), 0, length) for axis, length in enumerate(values.shape)]
        where[longest] = (where[longest] + shift) % values.shape[longest]
        spots.append(tuple(where))
    return values.at[spots[0]].set(least).at[spots[1]].set(largest)


def levels(own_key, extent, pieces, low, high):
    factor_of, own = 1.0, jax.random.fold_in(own_key, 6)
    for axis_at, blocks in pieces:
        draws = jnp.exp(jax.random.uniform(jax.random.fold_in(own, axis_at), (blocks,), jnp.float32, low / len(pieces), high / len(pieces)))
        factor_of = factor_of * jnp.repeat(draws, extent[axis_at] // blocks).reshape([-1 if axis == axis_at else 1 for axis in range(len(extent))])
    return factor_of


def scatter_about(key, extent, width, limit, pieces=(), kind=jnp.bfloat16):
    drawn = width * jax.random.normal(key, extent, jnp.float32)
    if pieces:
        drawn = drawn * levels(key, extent, pieces, -0.22, 0.18)
    return jnp.clip(drawn, -limit, limit).astype(kind)


def setup_inputs(seed: int = 0) -> dict:
    key_of = jax.random.split(jax.random.key(seed), 6)
    return {
        "profiles": scatter_about(key_of[0], (COLUMNS, 2 * NZ), 1.0, 6.0, ((0, 64),), jnp.float32),
        "courant": jnp.clip(jax.random.uniform(key_of[1], (COLUMNS, NZ), jnp.float32, -0.7, 0.7) * levels(key_of[1], (COLUMNS, NZ), ((0, 64),), -0.4, 0.0), -0.7, 0.7),
        "owner_map": draw_owner_map(jax.random.fold_in(key_of[5], 71), 0),
        "cloud_flags": with_ends((jax.random.randint(key_of[3], (COLUMNS,), 0, 2) < 1).astype(jnp.int32), jax.random.fold_in(key_of[3], 1), 0, 1),
        "crm_state": scatter_about(key_of[4], (2, NZ, NX, COLUMNS), 1.0, 6.0, ((2, 16), (3, 64)), jnp.float32),
    }


diffuse_x = 0.25
diffuse_z = 0.2
sat_scale = 0.5
sat_slope = 0.3
cond_rate = 0.5
latent_gain = 0.4


def condense(fields, cloudy):
    energy = fields[0]
    moisture = fields[1]
    saturation = sat_scale * (jnp.exp(sat_slope * energy) - 1.0)
    amount = cond_rate * jnp.maximum(moisture - saturation, 0.0) * cloudy
    return jnp.stack([energy + latent_gain * amount, moisture - amount])


def advance(centre, eastern, western, courant_here, forcing, cloudy):
    upper = jnp.concatenate([centre[:, 1:], centre[:, -1:]], axis=1)
    lower = jnp.concatenate([centre[:, :1], centre[:, :-1]], axis=1)
    stepped = centre + courant_here * ((western - eastern) * 0.5) + diffuse_x * (eastern - 2.0 * centre + western) + diffuse_z * (upper - 2.0 * centre + lower) + forcing
    return condense(stepped, cloudy)


def reference(profiles, courant, owner_map, cloud_flags, crm_state):
    columns = profiles.shape[0]
    phys_prof = jnp.zeros_like(profiles).at[owner_map].set(profiles)
    phys_cour = jnp.zeros_like(courant).at[owner_map].set(courant)
    forcing = (phys_prof.reshape(columns, 2, NZ).transpose(1, 2, 0) / STEPS)[:, :, None, :]
    courant_here = phys_cour.T[None, :, None, :]
    cloudy = cloud_flags.astype(jnp.float32)
    crm_now = crm_state
    for repeat in range(STEPS):
        crm_now = advance(crm_now, jnp.roll(crm_now, -1, axis=2), jnp.roll(crm_now, 1, axis=2), courant_here, forcing, cloudy)
    increment = (jnp.sum(crm_now, axis=2) - jnp.sum(crm_state, axis=2)) / NX
    phys_inc = increment.transpose(2, 0, 1).reshape(columns, 2 * NZ)
    tendency = phys_inc[owner_map]
    return tendency, crm_now
```

```python
import jax
import jax.numpy as jnp
from jax import lax
from jax.sharding import PartitionSpec as P

STEPS = 8


diffuse_x = 0.25
diffuse_z = 0.2
sat_scale = 0.5
sat_slope = 0.3
cond_rate = 0.5
latent_gain = 0.4


def sent_together(arrays, axis, split_dim, concat_dim, along):
    ends, at = ([], 0)
    for a in arrays[:-1]:
        at += a.shape[along]
        ends.append(at)
    both = jnp.concatenate(arrays, axis=along)
    return tuple(
        jnp.split(
            lax.all_to_all(both, axis, split_axis=split_dim, concat_axis=concat_dim, tiled=True),
            ends,
            axis=along,
        )
    )


def shifted(x, by):
    peers = lax.axis_size("grp")
    return lax.ppermute(x, "grp", [(i, (i + by) % peers) for i in range(peers)])


def condense(fields, cloudy):
    energy = fields[0]
    moisture = fields[1]
    saturation = sat_scale * (jnp.exp(sat_slope * energy) - 1.0)
    amount = cond_rate * jnp.maximum(moisture - saturation, 0.0) * cloudy
    return jnp.stack([energy + latent_gain * amount, moisture - amount])


def advance(widened, courant_here, forcing, cloudy):
    centre = widened[:, :, 1:-1]
    eastern = widened[:, :, 2:]
    western = widened[:, :, :-2]
    upper = jnp.concatenate([centre[:, 1:], centre[:, -1:]], axis=1)
    lower = jnp.concatenate([centre[:, :1], centre[:, :-1]], axis=1)
    stepped = (
        centre
        + courant_here * ((western - eastern) * 0.5)
        + diffuse_x * (eastern - 2.0 * centre + western)
        + diffuse_z * (upper - 2.0 * centre + lower)
        + forcing
    )
    return condense(stepped, cloudy)


def on_device(profiles, courant, owner_map, cloud_flags, crm_state):
    columns = profiles.shape[0]
    levels = courant.shape[1]
    col_count = lax.axis_size("col")
    col_index = lax.axis_index("col")
    per_peer = columns // col_count
    capacity = per_peer + min(2, per_peer)
    positions = jnp.arange(columns, dtype=jnp.int32)
    my_owner = lax.dynamic_slice_in_dim(owner_map, col_index * columns, columns)
    target = my_owner // columns
    earlier = (target[:, None] == target[None, :]) & (positions[None, :] < positions[:, None])
    order_in = jnp.sum(earlier.astype(jnp.int32), axis=1)
    sent_slot = target * capacity + order_in
    send_rows = jnp.full((col_count * capacity,), columns, jnp.int32).at[sent_slot].set(positions)
    padded_prof = jnp.concatenate([profiles, jnp.zeros((1, profiles.shape[1]), jnp.float32)])
    padded_cour = jnp.concatenate([courant, jnp.zeros((1, levels), jnp.float32)])
    out_prof = padded_prof[send_rows].reshape(col_count, capacity, profiles.shape[1])
    out_cour = padded_cour[send_rows].reshape(col_count, capacity, levels)
    got_prof, got_cour = sent_together((out_prof, out_cour), "col", 0, 0, 2)
    block_view = owner_map.reshape(col_count, columns)
    landing = (block_view // columns == col_index).astype(jnp.int32)
    before = jnp.cumsum(landing, axis=1) - landing
    sources = jnp.arange(col_count, dtype=jnp.int32)[:, None]
    where_from = sources * capacity + before
    landing_slot = jnp.where(landing > 0, block_view - col_index * columns, columns)
    senders_block = 4
    slot_blocks = landing_slot.reshape(col_count // senders_block, senders_block * columns)
    from_blocks = where_from.reshape(col_count // senders_block, senders_block * columns)

    def match_block(found, pair):
        slots, anchors = pair
        hits = slots[None, :] == positions[:, None]
        return (found + jnp.sum(jnp.where(hits, anchors[None, :], 0), axis=1), None)

    take_rows, unused = lax.scan(
        match_block, jnp.zeros((columns,), jnp.int32), (slot_blocks, from_blocks)
    )
    phys_prof = got_prof.reshape(col_count * capacity, profiles.shape[1])[take_rows]
    phys_cour = got_cour.reshape(col_count * capacity, levels)[take_rows]
    forcing = (phys_prof.reshape(columns, 2, levels).transpose(1, 2, 0) / STEPS)[:, :, None, :]
    courant_here = phys_cour.T[None, :, None, :]
    cloudy = cloud_flags.astype(jnp.float32)
    left_one = shifted(crm_state, 1)
    right_one = shifted(crm_state, -1)
    left_two = shifted(left_one, 1)
    right_two = shifted(right_one, -1)
    crm_now = jnp.concatenate([left_two, left_one, crm_state, right_one, right_two], axis=2)
    for repeat in range(STEPS):
        crm_now = advance(crm_now, courant_here, forcing, cloudy)
    pieces = lax.axis_size("grp")
    cells_all = crm_state.shape[2] * pieces
    partial_value = jnp.sum(crm_now, axis=2) - jnp.sum(crm_state, axis=2)
    share = -(-levels // pieces)
    spread = jnp.pad(partial_value, ((0, 0), (0, share * pieces - levels), (0, 0)))
    spread = spread.reshape(2, pieces, share, columns).transpose(1, 0, 2, 3)
    spread = spread.reshape(pieces, 2 * share, columns)
    totals = lax.all_to_all(spread, "grp", split_axis=0, concat_axis=0, tiled=True).sum(0)
    increment = totals / cells_all
    width = 2 * share
    back_rows = (
        jnp.zeros((col_count * capacity, width), jnp.float32).at[take_rows].set(increment.T)
    )
    got_back = lax.all_to_all(
        back_rows.reshape(col_count, 1, capacity * width),
        "col",
        split_axis=0,
        concat_axis=0,
        tiled=True,
    )
    my_share = got_back.reshape(col_count * capacity, width)[sent_slot].T
    copies = jnp.broadcast_to(my_share[None], (pieces, width, columns))
    every = lax.all_to_all(copies, "grp", split_axis=0, concat_axis=0, tiled=True)
    every = every.reshape(pieces, 2, share, columns).transpose(3, 1, 0, 2)
    tendency = every.reshape(columns, 2, pieces * share)[:, :, :levels]
    return (tendency.reshape(columns, 2 * levels), crm_now)


def solution(mesh):
    placed = (P("col", None), P("col", None), P(), P("col"), P(None, None, "grp", "col"))
    return jax.shard_map(
        on_device,
        mesh=mesh,
        in_specs=placed,
        out_specs=(P("col", None), P(None, None, "grp", "col")),
        check_vma=False,
    )
```

```python
import jax
import jax.numpy as jnp
from jax import lax
from jax.experimental import pallas as pl
from jax.experimental.pallas import tpu as pltpu
from jax.sharding import PartitionSpec as P

STEPS = 8

diffuse_x = 0.25
diffuse_z = 0.2
sat_scale = 0.5
sat_slope = 0.3
cond_rate = 0.5
latent_gain = 0.4

LANES = 128
LEVELS = 58
GROWTH = sat_slope * 1.4426950408889634
VMEM = pl.BlockSpec(memory_space=pltpu.VMEM)
SMEM = pl.BlockSpec(memory_space=pltpu.SMEM)


def thirds(x):
    first = x.astype(jnp.bfloat16)
    rest = x - first.astype(jnp.float32)
    second = rest.astype(jnp.bfloat16)
    third = (rest - second.astype(jnp.float32)).astype(jnp.bfloat16)
    return first, second, third


def dot(a, b, dims=((1,), (0,))):
    return lax.dot_general(a, b, (dims, ((), ())), preferred_element_type=jnp.float32)


def earlier(hits, count):
    row = lax.broadcasted_iota(jnp.int32, (count, count), 0)
    col = lax.broadcasted_iota(jnp.int32, (count, count), 1)
    strict = jnp.where(row < col, 1.0, 0.0).astype(jnp.bfloat16)
    return dot(jnp.where(hits, 1.0, 0.0).astype(jnp.bfloat16), strict)


def rows_of(owners, count):
    left = owners[pl.ds(0, count, stride=2), :]
    right = owners[pl.ds(1, count, stride=2), :]
    return jnp.concatenate([left, right], axis=1)


def pack_kernel(me, owners, prof, cour, packed, picks):
    feats, columns = prof.shape
    levels = cour.shape[0]
    peers = owners.shape[0] * LANES // columns
    slots = picks.shape[0] // peers
    tiles = packed.shape[0] // peers
    half = LANES // 2
    mine = [owners[pl.ds(2 * me[0] + i, 1), :] for i in range(2)]
    target = jnp.concatenate(mine, axis=1) // columns
    hits = lax.broadcasted_iota(jnp.int32, (peers, columns), 0) == target
    order = earlier(hits, columns)
    chosen = jnp.concatenate(
        [jnp.where(hits & (order == k), 1.0, 0.0) for k in range(slots)], axis=0
    ).astype(jnp.bfloat16)
    picks[...] = chosen
    gap = jnp.zeros((half - levels, columns), jnp.float32)
    wind = jnp.concatenate([cour[...], gap], axis=0)
    blank = jnp.zeros_like(wind)
    table = jnp.concatenate(
        [prof[...], jnp.zeros((LANES - feats, columns), jnp.float32), wind, blank, blank, wind],
        axis=0,
    )
    rows = sum(dot(chosen, piece, ((1,), (1,))) for piece in thirds(table))
    for k in range(slots):
        packed[pl.ds(k, peers, stride=tiles), :] = rows[k * peers : (k + 1) * peers, :LANES]
    for j in range(slots // 2):
        low = rows[2 * j * peers : (2 * j + 1) * peers, LANES : 2 * LANES]
        high = rows[(2 * j + 1) * peers : (2 * j + 2) * peers, 2 * LANES :]
        packed[pl.ds(slots + j, peers, stride=tiles), :] = low + high


def landing_kernel(me, owners, lands):
    columns = lands.shape[1]
    peers = owners.shape[0] * LANES // columns
    slots = lands.shape[0] // peers
    own = rows_of(owners, peers)
    hits = own // columns == me[0]
    order = earlier(hits, columns)
    local = (own % columns + 1).astype(jnp.float32)
    place = lax.broadcasted_iota(jnp.int32, (peers, columns), 1).astype(jnp.float32)
    for k in range(slots):
        spot = jnp.sum(jnp.where(hits & (order == k), local, 0.0), axis=1, keepdims=True)
        lands[k * peers : (k + 1) * peers, :] = jnp.where(spot - 1.0 == place, 1.0, 0.0).astype(
            jnp.bfloat16
        )


def forcing_kernel(got, lands, flags, force, east, west, rate):
    columns = lands.shape[1]
    fields, lane_tiles, tall, _ = force.shape
    slots = 6
    peers = lands.shape[0] // slots
    tiles = got.shape[0] // peers
    half = LANES // 2
    landed = lands[...]
    stacked = jnp.concatenate(
        [got[pl.ds(k, peers, stride=tiles), :] for k in range(slots)], axis=0
    )
    forcing = sum(dot(piece, landed) for piece in thirds(stacked.T)) / STEPS
    wind = jnp.zeros((half, columns), jnp.float32)
    for j in range(slots // 2):
        turned = thirds(got[pl.ds(slots + j, peers, stride=tiles), :].T)
        for odd in range(2):
            where_to = landed[(2 * j + odd) * peers : (2 * j + odd + 1) * peers]
            for piece in turned:
                wind = wind + dot(piece[odd * half : (odd + 1) * half], where_to)
    fraction = cond_rate * flags[...].astype(jnp.float32)
    fraction = jnp.broadcast_to(fraction, (8, columns))
    for c in range(lane_tiles):
        lanes = slice(c * LANES, (c + 1) * LANES)
        east[c] = diffuse_x - 0.5 * wind[:tall, lanes]
        west[c] = diffuse_x + 0.5 * wind[:tall, lanes]
        rate[0, c] = fraction[:, lanes]
        rate[1, c] = (latent_gain * GROWTH) * fraction[:, lanes]
        for f in range(fields):
            rows = forcing[f * LEVELS : (f + 1) * LEVELS, lanes]
            force[f, c, :LEVELS, :] = rows * GROWTH if f == 0 else rows


BLOCKS = ((1, 9, 11), (2, 10), (3, 9), (4, 8), (5, 7), (6,), (6,), (8,))
GROUPS = (2, 2, 2, 2, 2, 4, 4, 4)


def steps_kernel(
    force, east, west, rate, own, left1, right1, left2, right2, final, change, even, odd, sums
):
    fields, levels, lane_tiles, _, _ = even.shape
    slabs = (left2, left1, own, right1, right2)
    cells = 8 // lane_tiles
    share = change.shape[1] // fields
    sums[...] = jnp.zeros_like(sums)

    def place(z, carry):
        for f in range(fields):
            for c in range(lane_tiles):
                for s, slab in enumerate(slabs):
                    value = slab[f * levels + z, c * cells : (c + 1) * cells, :]
                    value = GROWTH * value - 1.0 if f == 0 else value + sat_scale
                    even[f, z, c, s * cells : (s + 1) * cells, :] = value
        return carry

    lax.fori_loop(0, levels, place, 0)
    rates = [[jnp.broadcast_to(rate[f, c, :1, :], (8, LANES)) for c in range(lane_tiles)] for f in range(2)]

    def at_level(step, source, z, below, above):
        results = []
        for c in range(lane_tiles):
            wide = [jnp.broadcast_to(w[c, pl.ds(z, 1), :], (8, LANES)) for w in (east, west)]
            push = [jnp.broadcast_to(force[f, c, pl.ds(z, 1), :], (8, LANES)) for f in range(fields)]
            for row in BLOCKS[step]:
                rows = slice(row, row + 8)
                stepped = []
                for f in range(fields):
                    stepped.append(
                        (1.0 - 2.0 * diffuse_x - 2.0 * diffuse_z) * source[f, z, c, rows, :]
                        + diffuse_z * (source[f, below, c, rows, :] + source[f, above, c, rows, :])
                        + (
                            wide[0] * source[f, z, c, row + 1 : row + 9, :]
                            + wide[1] * source[f, z, c, row - 1 : row + 7, :]
                        )
                        + push[f]
                    )
                energy, moisture = stepped
                excess = jnp.maximum(moisture - jnp.exp2(energy), 0.0)
                results.append((c, row, energy + rates[1][c] * excess, moisture - rates[0][c] * excess))
        return results

    def store(step, target, z, results):
        for c, row, energy, moisture in results:
            if step < STEPS - 1:
                target[0, z, c, row : row + 8, :] = energy
                target[1, z, c, row : row + 8, :] = moisture
                continue
            energy = (energy + 1.0) * (1.0 / GROWTH)
            moisture = moisture - sat_scale
            for f, now in enumerate((energy, moisture)):
                now = now[:cells]
                start = own[f * levels + z, c * cells : (c + 1) * cells, :]
                final[f * levels + z, c * cells : (c + 1) * cells, :] = now
                sums[f, c, pl.ds(z, 1), :] = jnp.sum(now - start, axis=0, keepdims=True)

    for step in range(STEPS):
        source, target = (even, odd) if step % 2 == 0 else (odd, even)
        many = GROUPS[step]

        def body(i, carry, step=step, source=source, target=target, many=many):
            zs = [i * many + k for k in range(many)]
            found = [
                at_level(step, source, z, jnp.maximum(z - 1, 0), jnp.minimum(z + 1, levels - 1))
                for z in zs
            ]
            for z, results in zip(zs, found):
                store(step, target, z, results)
            return carry

        lax.fori_loop(0, levels // many, body, 0)
        for z in range(levels // many * many, levels):
            store(step, target, z, at_level(step, source, z, max(z - 1, 0), min(z + 1, levels - 1)))
    for f in range(fields):
        for c in range(lane_tiles):
            for g in range(change.shape[0]):
                change[g, f * share : (f + 1) * share, c * LANES : (c + 1) * LANES] = sums[
                    f, c, g * share : (g + 1) * share, :
                ]


def return_kernel(inverse, parts, lands, sent):
    pieces, rows, columns = parts.shape
    peers = sent.shape[0]
    slots = lands.shape[0] // peers
    total = parts[0]
    for g in range(1, pieces):
        total = total + parts[g]
    total = total * inverse[0]
    many = jnp.concatenate([total] * (LANES // rows), axis=0)
    placed = sum(dot(lands[...], piece, ((1,), (1,))) for piece in thirds(many))
    lane = lax.broadcasted_iota(jnp.int32, (peers, LANES), 1) // rows
    out = jnp.zeros((peers, LANES), jnp.float32)
    for k in range(slots):
        out = out + jnp.where(lane == k, placed[k * peers : (k + 1) * peers], 0.0)
    sent[...] = out


def arrive_kernel(got, picks, copies):
    peers = got.shape[0]
    slots = picks.shape[0] // peers
    pieces, rows, columns = copies.shape
    turned = thirds(got[...].T)
    share = jnp.zeros((rows, columns), jnp.float32)
    for k in range(slots):
        where_to = picks[k * peers : (k + 1) * peers]
        for piece in turned:
            share = share + dot(piece, where_to)[k * rows : (k + 1) * rows]
    for g in range(pieces):
        copies[g] = share


def spread_kernel(every, tendency):
    pieces, rows, columns = every.shape
    share = rows // 2
    levels = tendency.shape[0] // 2
    for f in range(2):
        for g in range(pieces):
            here = min(share, levels - g * share)
            if here > 0:
                start = f * levels + g * share
                tendency[start : start + here, :] = every[g, f * share : f * share + here, :]


def call(kernel, outs, scratch=(), scalars=0, inputs=0):
    return pl.pallas_call(
        kernel,
        out_shape=outs,
        in_specs=[SMEM] * scalars + [VMEM] * inputs,
        out_specs=jax.tree.map(lambda _: VMEM, outs),
        scratch_shapes=list(scratch),
        compiler_params=pltpu.CompilerParams(vmem_limit_bytes=16 * 1024 * 1024),
    )


def shifted(x, by):
    peers = lax.axis_size("grp")
    return lax.ppermute(x, "grp", [(i, (i + by) % peers) for i in range(peers)])


def traded(x, axis):
    return lax.all_to_all(x, axis, split_axis=0, concat_axis=0, tiled=True)


def flat(x):
    f, z, cells, columns = x.shape
    x = x.reshape(f, z, cells, columns // LANES, LANES).transpose(0, 1, 3, 2, 4)
    return x.reshape(f * z, cells * columns // LANES, LANES)


def on_device(profiles, courant, owner_map, cloud_flags, crm_state):
    columns, feats = profiles.shape
    levels = courant.shape[1]
    col_count = lax.axis_size("col")
    pieces = lax.axis_size("grp")
    fields, _, cells, _ = crm_state.shape
    per_peer = columns // col_count
    capacity = per_peer + min(2, per_peer)
    share = -(-levels // pieces)
    tall = share * pieces
    lane_tiles = columns // LANES
    f32, bf16 = jnp.float32, jnp.bfloat16
    S = jax.ShapeDtypeStruct
    me = lax.axis_index("col").reshape(1)
    owners = owner_map.reshape(-1, LANES)
    left1, right1 = shifted(crm_state, 1), shifted(crm_state, -1)
    tiles = capacity + capacity // 2
    packed, picks = call(
        pack_kernel,
        (S((col_count * tiles, LANES), f32), S((capacity * col_count, columns), bf16)),
        (),
        1,
        3,
    )(me, owners, profiles.T, courant.T)
    got = traded(packed.reshape(col_count, 1, tiles * LANES), "col").reshape(packed.shape)
    lands = call(landing_kernel, S((capacity * col_count, columns), bf16), (), 1, 1)(me, owners)
    left2, right2 = shifted(left1, 1), shifted(right1, -1)
    forces = call(
        forcing_kernel,
        (
            S((fields, lane_tiles, tall, LANES), f32),
            S((lane_tiles, tall, LANES), f32),
            S((lane_tiles, tall, LANES), f32),
            S((2, lane_tiles, 8, LANES), f32),
        ),
        (),
        0,
        3,
    )(got, lands, cloud_flags.reshape(1, columns))
    slabs = [flat(x) for x in (crm_state, left1, right1, left2, right2)]
    rows, change = call(
        steps_kernel,
        (S(slabs[0].shape, f32), S((pieces, 2 * share, columns), f32)),
        [pltpu.VMEM((fields, levels, lane_tiles, 24, LANES), f32)] * 2
        + [pltpu.VMEM((fields, lane_tiles, tall, LANES), f32)],
        0,
        9,
    )(*forces, *slabs)
    rows = rows.reshape(fields, levels, lane_tiles, cells, LANES).transpose(0, 1, 3, 2, 4)
    crm_final = rows.reshape(crm_state.shape)
    parts = traded(change, "grp")
    inverse = jnp.full((1,), 1.0 / (pieces * cells), f32)
    back = call(return_kernel, S((col_count, LANES), f32), (), 1, 2)(inverse, parts, lands)
    back = traded(back.reshape(col_count, 1, LANES), "col").reshape(back.shape)
    copies = call(arrive_kernel, S((pieces, 2 * share, columns), f32), (), 0, 2)(back, picks)
    every = traded(copies, "grp")
    tendency = call(spread_kernel, S((feats, columns), f32), (), 0, 1)(every)
    return tendency.T, crm_final


def solution(mesh):
    placed = (P("col", None), P("col", None), P(), P("col"), P(None, None, "grp", "col"))
    return jax.shard_map(
        on_device,
        mesh=mesh,
        in_specs=placed,
        out_specs=(P("col", None), P(None, None, "grp", "col")),
        check_vma=False,
    )
```

```python
import functools

import jax
import jax.numpy as jnp
from jax import lax
from jax.experimental import pallas as pl
from jax.experimental.pallas import tpu as pltpu
from jax.sharding import PartitionSpec as P

STEPS = 8

diffuse_x = 0.25
diffuse_z = 0.2
sat_scale = 0.5
sat_slope = 0.3
cond_rate = 0.5
latent_gain = 0.4

LANES = 128
GROWTH = sat_slope * 1.4426950408889634
VMEM = pl.BlockSpec(memory_space=pltpu.VMEM)
SMEM = pl.BlockSpec(memory_space=pltpu.SMEM)


def thirds(x):
    first = x.astype(jnp.bfloat16)
    rest = x - first.astype(jnp.float32)
    second = rest.astype(jnp.bfloat16)
    third = (rest - second.astype(jnp.float32)).astype(jnp.bfloat16)
    return first, second, third


def dot(a, b, dims=((1,), (0,))):
    return lax.dot_general(a, b, (dims, ((), ())), preferred_element_type=jnp.float32)


def earlier(hits, count):
    row = lax.broadcasted_iota(jnp.int32, (count, count), 0)
    col = lax.broadcasted_iota(jnp.int32, (count, count), 1)
    strict = jnp.where(row < col, 1.0, 0.0).astype(jnp.bfloat16)
    return dot(jnp.where(hits, 1.0, 0.0).astype(jnp.bfloat16), strict)


def rows_of(owners, count):
    left = owners[pl.ds(0, count, stride=2), :]
    right = owners[pl.ds(1, count, stride=2), :]
    return jnp.concatenate([left, right], axis=1)


def pack_kernel(me, owners, prof, cour, packed, picks):
    feats, columns = prof.shape
    levels = cour.shape[0]
    peers = owners.shape[0] * LANES // columns
    slots = picks.shape[0] // peers
    tiles = packed.shape[0] // peers
    half = LANES // 2
    mine = [owners[pl.ds(2 * me[0] + i, 1), :] for i in range(2)]
    target = jnp.concatenate(mine, axis=1) // columns
    hits = lax.broadcasted_iota(jnp.int32, (peers, columns), 0) == target
    order = earlier(hits, columns)
    chosen = jnp.concatenate(
        [jnp.where(hits & (order == k), 1.0, 0.0) for k in range(slots)], axis=0
    ).astype(jnp.bfloat16)
    picks[...] = chosen
    gap = jnp.zeros((half - levels, columns), jnp.float32)
    wind = jnp.concatenate([cour[...], gap], axis=0)
    blank = jnp.zeros_like(wind)
    table = jnp.concatenate(
        [prof[...], jnp.zeros((LANES - feats, columns), jnp.float32), wind, blank, blank, wind],
        axis=0,
    )
    rows = sum(dot(chosen, piece, ((1,), (1,))) for piece in thirds(table))
    for k in range(slots):
        packed[pl.ds(k, peers, stride=tiles), :] = rows[k * peers : (k + 1) * peers, :LANES]
    for j in range(slots // 2):
        low = rows[2 * j * peers : (2 * j + 1) * peers, LANES : 2 * LANES]
        high = rows[(2 * j + 1) * peers : (2 * j + 2) * peers, 2 * LANES :]
        packed[pl.ds(slots + j, peers, stride=tiles), :] = low + high


def landing_kernel(me, owners, lands):
    columns = lands.shape[1]
    peers = owners.shape[0] * LANES // columns
    slots = lands.shape[0] // peers
    own = rows_of(owners, peers)
    hits = own // columns == me[0]
    order = earlier(hits, columns)
    local = (own % columns + 1).astype(jnp.float32)
    place = lax.broadcasted_iota(jnp.int32, (peers, columns), 1).astype(jnp.float32)
    for k in range(slots):
        spot = jnp.sum(jnp.where(hits & (order == k), local, 0.0), axis=1, keepdims=True)
        lands[k * peers : (k + 1) * peers, :] = jnp.where(spot - 1.0 == place, 1.0, 0.0).astype(
            jnp.bfloat16
        )


def forcing_kernel(got, lands, flags, force, east, west, rate, rows):
    columns = lands.shape[1]
    tiles = 9
    peers = got.shape[0] // tiles
    slots = lands.shape[0] // peers
    levels = east.shape[0]
    lane_tiles = rows.shape[0]
    half = LANES // 2
    landed = lands[...]
    stacked = jnp.concatenate(
        [got[pl.ds(k, peers, stride=tiles), :] for k in range(slots)], axis=0
    )
    forcing = sum(dot(piece, landed) for piece in thirds(stacked.T)) / STEPS
    wind = jnp.zeros((half, columns), jnp.float32)
    for j in range(slots // 2):
        turned = thirds(got[pl.ds(slots + j, peers, stride=tiles), :].T)
        for odd in range(2):
            where_to = landed[(2 * j + odd) * peers : (2 * j + odd + 1) * peers]
            for piece in turned:
                wind = wind + dot(piece[odd * half : (odd + 1) * half], where_to)
    for c in range(lane_tiles):
        lanes = slice(c * LANES, (c + 1) * LANES)
        rows[c, :LANES, :] = forcing[:, lanes]
        rows[c, LANES:, :] = 0.5 * wind[:, lanes]
    even = lax.broadcasted_iota(jnp.int32, (8, LANES), 0) % 2 == 0

    def woven(line):
        first, second = (jnp.broadcast_to(rows[c, pl.ds(line, 1), :], (8, LANES)) for c in (0, 1))
        return jnp.where(even, first, second)

    def weave(z, carry):
        force[z] = GROWTH * woven(z)
        force[levels + z] = woven(levels + z)
        along = woven(LANES + z)
        east[z] = diffuse_x - along
        west[z] = diffuse_x + along
        return carry

    lax.fori_loop(0, levels, weave, 0, unroll=2)
    fraction = cond_rate * flags[...].astype(jnp.float32)
    first, second = (
        jnp.broadcast_to(fraction[:, c * LANES : (c + 1) * LANES], (8, LANES)) for c in (0, 1)
    )
    fraction = jnp.where(even, first, second)
    rate[0] = (latent_gain * GROWTH) * fraction
    rate[1] = fraction


def place(slab, first, target, z):
    levels = target.shape[0] // 2
    for f in range(2):
        for c in range(2):
            value = slab[f * levels + z, 4 * c : 4 * c + 4, :]
            value = GROWTH * value - 1.0 if f == 0 else value + sat_scale
            target[f * levels + z, pl.ds(2 * first + c, 4, stride=2), :] = value


def march(force, east, west, rates, source, z, below, above, starts):
    levels = east.shape[0]
    results = []
    for row in starts:
        stepped = []
        for f in range(2):
            base = f * levels
            stepped.append(
                (1.0 - 2.0 * diffuse_x - 2.0 * diffuse_z) * source[base + z, row : row + 8, :]
                + diffuse_z
                * (source[base + below, row : row + 8, :] + source[base + above, row : row + 8, :])
                + (
                    east[z] * source[base + z, row + 2 : row + 10, :]
                    + west[z] * source[base + z, row - 2 : row + 6, :]
                )
                + force[base + z]
            )
        energy, moisture = stepped
        excess = jnp.maximum(moisture - jnp.exp2(energy), 0.0)
        results.append((energy + rates[0] * excess, moisture - rates[1] * excess))
    return results


def sweep(levels, many, work, keep):
    def body(i, carry):
        zs = [i * many + k for k in range(many)]
        found = [work(z, jnp.maximum(z - 1, 0), jnp.minimum(z + 1, levels - 1)) for z in zs]
        for z, results in zip(zs, found):
            keep(z, results)
        return carry

    lax.fori_loop(0, levels // many, body, 0)
    for z in range(levels // many * many, levels):
        keep(z, work(z, max(z - 1, 0), min(z + 1, levels - 1)))


NARROW = ((10, 18, 22), (12, 20), (14, 18), (16,))
MANY = (9, 29, 29, 29)


def inner_kernel(parity, force, east, west, rate, own, near0, near1, edges, even, odd):
    levels = east.shape[0]
    rates = (rate[0], rate[1])

    def fill(left, right):
        def body(z, carry):
            for slab, first in ((left, 4), (own, 8), (right, 12)):
                place(slab, first, even, z)
            return carry

        lax.fori_loop(0, levels, body, 0, unroll=2)

    @pl.when(parity[0] == 0)
    def _():
        fill(near1, near0)

    @pl.when(parity[0] == 1)
    def _():
        fill(near0, near1)

    def copy_edges(t, source):
        def body(i, carry):
            edges[t, i, 0:4, :] = source[i, 8 + 2 * t : 12 + 2 * t, :]
            edges[t, i, 4:8, :] = source[i, 28 - 2 * t : 32 - 2 * t, :]
            if t == 0:
                edges[5, i] = source[i, 16:24, :]
            return carry

        lax.fori_loop(0, 2 * levels, body, 0, unroll=4)

    copy_edges(0, even)
    for t, starts in enumerate(NARROW):
        source, target = (even, odd) if t % 2 == 0 else (odd, even)

        def keep(z, results, target=target, starts=starts):
            for row, pair in zip(starts, results):
                for f, value in enumerate(pair):
                    target[f * levels + z, row : row + 8, :] = value

        def work(z, below, above, source=source, starts=starts):
            return march(force, east, west, rates, source, z, below, above, starts)

        sweep(levels, MANY[t], work, keep)
        copy_edges(t + 1, target)


def outer_kernel(parity, force, east, west, rate, far0, far1, edges, ended, change, even, odd, sums):
    levels = east.shape[0]
    rates = (rate[0], rate[1])
    share = change.shape[1] // 2
    sums[...] = jnp.zeros_like(sums)

    def fill(left, right):
        def body(z, carry):
            place(left, 0, even, z)
            place(right, 16, even, z)
            for f in range(2):
                i = f * levels + z
                even[i, 8:12, :] = edges[0, i, 0:4, :]
                even[i, 28:32, :] = edges[0, i, 4:8, :]
            return carry

        lax.fori_loop(0, levels, body, 0, unroll=2)

    @pl.when(parity[0] == 0)
    def _():
        fill(far1, far0)

    @pl.when(parity[0] == 1)
    def _():
        fill(far0, far1)

    for t in range(4):
        source, target = (even, odd) if t % 2 == 0 else (odd, even)
        starts = (2 * t + 2, 30 - 2 * t)

        def keep(z, results, t=t, target=target, starts=starts):
            for f in range(2):
                i = f * levels + z
                for row, pair in zip(starts, results):
                    target[i, row : row + 8, :] = pair[f]
                target[i, 10 + 2 * t : 14 + 2 * t, :] = edges[t + 1, i, 0:4, :]
                target[i, 26 - 2 * t : 30 - 2 * t, :] = edges[t + 1, i, 4:8, :]

        def work(z, below, above, source=source, starts=starts):
            return march(force, east, west, rates, source, z, below, above, starts)

        sweep(levels, 29, work, keep)
    for t, starts in enumerate(NARROW):
        source, target = (even, odd) if t % 2 == 0 else (odd, even)

        def keep(z, results, t=t, target=target, starts=starts):
            for row, pair in zip(starts, results):
                for f, value in enumerate(pair):
                    i = f * levels + z
                    if t < len(NARROW) - 1:
                        target[i, row : row + 8, :] = value
                        continue
                    grown = value - edges[5, i]
                    ended[i] = (value + 1.0) * (1.0 / GROWTH) if f == 0 else value - sat_scale
                    grown = grown + pltpu.roll(grown, 2, 0)
                    grown = grown + pltpu.roll(grown, 4, 0)
                    for c in range(2):
                        sums[f, c, pl.ds(z, 1), :] = grown[c : c + 1, :]

        def work(z, below, above, source=source, starts=starts):
            return march(force, east, west, rates, source, z, below, above, starts)

        sweep(levels, MANY[t], work, keep)

    for f in range(2):
        scale = 1.0 / GROWTH if f == 0 else 1.0
        for c in range(2):
            for g in range(change.shape[0]):
                change[g, f * share : (f + 1) * share, c * LANES : (c + 1) * LANES] = (
                    scale * sums[f, c, g * share : (g + 1) * share, :]
                )


def finish_kernel(ended, final):
    def body(i, carry):
        for c in range(2):
            final[i, 4 * c : 4 * c + 4, :] = ended[i, pl.ds(c, 4, stride=2), :]
        return carry

    lax.fori_loop(0, final.shape[0], body, 0, unroll=4)


def return_kernel(inverse, parts, lands, sent):
    pieces, rows, columns = parts.shape
    peers = sent.shape[0]
    slots = lands.shape[0] // peers
    total = parts[0]
    for g in range(1, pieces):
        total = total + parts[g]
    total = total * inverse[0]
    many = jnp.concatenate([total] * (LANES // rows), axis=0)
    placed = sum(dot(lands[...], piece, ((1,), (1,))) for piece in thirds(many))
    lane = lax.broadcasted_iota(jnp.int32, (peers, LANES), 1) // rows
    out = jnp.zeros((peers, LANES), jnp.float32)
    for k in range(slots):
        out = out + jnp.where(lane == k, placed[k * peers : (k + 1) * peers], 0.0)
    sent[...] = out


def arrive_kernel(got, picks, copies):
    peers = got.shape[0]
    slots = picks.shape[0] // peers
    pieces, rows, columns = copies.shape
    turned = thirds(got[...].T)
    share = jnp.zeros((rows, columns), jnp.float32)
    for k in range(slots):
        where_to = picks[k * peers : (k + 1) * peers]
        for piece in turned:
            share = share + dot(piece, where_to)[k * rows : (k + 1) * rows]
    for g in range(pieces):
        copies[g] = share


def spread_kernel(every, tendency):
    pieces, rows, columns = every.shape
    share = rows // 2
    levels = tendency.shape[0] // 2
    for f in range(2):
        for g in range(pieces):
            here = min(share, levels - g * share)
            if here > 0:
                start = f * levels + g * share
                tendency[start : start + here, :] = every[g, f * share : f * share + here, :]


def call(kernel, outs, scratch=(), scalars=0, inputs=0, limit=16):
    return pl.pallas_call(
        kernel,
        out_shape=outs,
        in_specs=[SMEM] * scalars + [VMEM] * inputs,
        out_specs=jax.tree.map(lambda _: VMEM, outs),
        scratch_shapes=list(scratch),
        compiler_params=pltpu.CompilerParams(vmem_limit_bytes=limit * 1024 * 1024),
    )


def swapped(x, odd):
    peers = lax.axis_size("grp")
    return lax.ppermute(
        x, "grp", [(i, (i + 1 if i % 2 == odd else i - 1) % peers) for i in range(peers)]
    )


def traded(x, axis):
    return lax.all_to_all(x, axis, split_axis=0, concat_axis=0, tiled=True)


def flat(x):
    f, z, cells, columns = x.shape
    x = x.reshape(f, z, cells, columns // LANES, LANES).transpose(0, 1, 3, 2, 4)
    return x.reshape(f * z, cells * columns // LANES, LANES)


def on_device(profiles, courant, owner_map, cloud_flags, crm_state):
    columns, feats = profiles.shape
    levels = courant.shape[1]
    col_count = lax.axis_size("col")
    pieces = lax.axis_size("grp")
    fields, _, cells, _ = crm_state.shape
    per_peer = columns // col_count
    capacity = per_peer + min(2, per_peer)
    share = -(-levels // pieces)
    tall = share * pieces
    lane_tiles = columns // LANES
    f32, bf16 = jnp.float32, jnp.bfloat16
    S = jax.ShapeDtypeStruct
    me = lax.axis_index("col").reshape(1)
    owners = owner_map.reshape(-1, LANES)
    near0, near1 = swapped(crm_state, 0), swapped(crm_state, 1)
    tiles = capacity + capacity // 2
    packed, picks = call(
        pack_kernel,
        (S((col_count * tiles, LANES), f32), S((capacity * col_count, columns), bf16)),
        (),
        1,
        3,
        60,
    )(me, owners, profiles.T, courant.T)
    got = traded(packed.reshape(col_count, 1, tiles * LANES), "col").reshape(packed.shape)
    lands = call(landing_kernel, S((capacity * col_count, columns), bf16), (), 1, 1)(me, owners)
    far0, far1 = swapped(near1, 0), swapped(near0, 1)
    lines = fields * levels
    forces = call(
        forcing_kernel,
        (
            S((lines, 8, LANES), f32),
            S((levels, 8, LANES), f32),
            S((levels, 8, LANES), f32),
            S((2, 8, LANES), f32),
        ),
        [pltpu.VMEM((lane_tiles, 3 * LANES // 2, LANES), f32)],
        0,
        3,
    )(got, lands, cloud_flags.reshape(1, columns))
    parity = (lax.axis_index("grp") % 2).reshape(1)
    own = flat(crm_state)
    state = pltpu.VMEM((lines, 40, LANES), f32)
    edges = call(inner_kernel, S((6, lines, 8, LANES), f32), [state, state], 1, 7)(
        parity, *forces, own, flat(near0), flat(near1)
    )
    ended, change = call(
        outer_kernel,
        (S(own.shape, f32), S((pieces, 2 * share, columns), f32)),
        [state, state, pltpu.VMEM((fields, lane_tiles, tall, LANES), f32)],
        1,
        7,
    )(parity, *forces, flat(far0), flat(far1), edges)
    rows = call(finish_kernel, S(own.shape, f32), (), 0, 1)(ended)
    rows = rows.reshape(fields, levels, lane_tiles, cells, LANES).transpose(0, 1, 3, 2, 4)
    crm_final = rows.reshape(crm_state.shape)
    parts = traded(change, "grp")
    inverse = jnp.full((1,), 1.0 / (pieces * cells), f32)
    back = call(return_kernel, S((col_count, LANES), f32), (), 1, 2)(inverse, parts, lands)
    back = traded(back.reshape(col_count, 1, LANES), "col").reshape(back.shape)
    copies = call(arrive_kernel, S((pieces, 2 * share, columns), f32), (), 0, 2)(back, picks)
    every = traded(copies, "grp")
    tendency = call(spread_kernel, S((feats, columns), f32), (), 0, 1)(every)
    return tendency.T, crm_final


def solution(mesh):
    placed = (P("col", None), P("col", None), P(), P("col"), P(None, None, "grp", "col"))
    return jax.shard_map(
        on_device,
        mesh=mesh,
        in_specs=placed,
        out_specs=(P("col", None), P(None, None, "grp", "col")),
        check_vma=False,
    )
```

```python
import functools

import jax
import jax.numpy as jnp
from jax import lax
from jax.experimental import pallas as pl
from jax.experimental.pallas import tpu as pltpu
from jax.sharding import PartitionSpec as P

STEPS = 8

diffuse_x = 0.25
diffuse_z = 0.2
sat_scale = 0.5
sat_slope = 0.3
cond_rate = 0.5
latent_gain = 0.4

LANES = 128
GROWTH = sat_slope * 1.4426950408889634
VMEM = pl.BlockSpec(memory_space=pltpu.VMEM)
SMEM = pl.BlockSpec(memory_space=pltpu.SMEM)


def thirds(x):
    first = x.astype(jnp.bfloat16)
    rest = x - first.astype(jnp.float32)
    second = rest.astype(jnp.bfloat16)
    third = (rest - second.astype(jnp.float32)).astype(jnp.bfloat16)
    return first, second, third


def dot(a, b, dims=((1,), (0,))):
    return lax.dot_general(a, b, (dims, ((), ())), preferred_element_type=jnp.float32)


def earlier(hits, count):
    row = lax.broadcasted_iota(jnp.int32, (count, count), 0)
    col = lax.broadcasted_iota(jnp.int32, (count, count), 1)
    strict = jnp.where(row < col, 1.0, 0.0).astype(jnp.bfloat16)
    return dot(jnp.where(hits, 1.0, 0.0).astype(jnp.bfloat16), strict)


def rows_of(owners, count):
    left = owners[pl.ds(0, count, stride=2), :]
    right = owners[pl.ds(1, count, stride=2), :]
    return jnp.concatenate([left, right], axis=1)


def chosen_slots(me, owners, peers, slots):
    mine = [owners[pl.ds(2 * me[0] + i, 1), :] for i in range(2)]
    mine = jnp.concatenate(mine, axis=1)
    columns = mine.shape[1]
    hits = lax.broadcasted_iota(jnp.int32, (peers, columns), 0) == mine // columns
    order = earlier(hits, columns)
    return jnp.concatenate(
        [jnp.where(hits & (order == k), 1.0, 0.0) for k in range(slots)], axis=0
    ).astype(jnp.bfloat16)


def pack_kernel(me, owners, prof, cour, packed):
    feats, columns = prof.shape
    levels = cour.shape[0]
    peers = owners.shape[0] * LANES // columns
    tiles = packed.shape[0] // peers
    slots = tiles * 2 // 3
    half = LANES // 2
    chosen = chosen_slots(me, owners, peers, slots)
    gap = jnp.zeros((half - levels, columns), jnp.float32)
    wind = jnp.concatenate([cour[...], gap], axis=0)
    blank = jnp.zeros_like(wind)
    table = jnp.concatenate(
        [prof[...], jnp.zeros((LANES - feats, columns), jnp.float32), wind, blank, blank, wind],
        axis=0,
    )
    rows = sum(dot(chosen, piece, ((1,), (1,))) for piece in thirds(table))
    for k in range(slots):
        packed[pl.ds(k, peers, stride=tiles), :] = rows[k * peers : (k + 1) * peers, :LANES]
    for j in range(slots // 2):
        low = rows[2 * j * peers : (2 * j + 1) * peers, LANES : 2 * LANES]
        high = rows[(2 * j + 1) * peers : (2 * j + 2) * peers, 2 * LANES :]
        packed[pl.ds(slots + j, peers, stride=tiles), :] = low + high


def landing_kernel(me, owners, flags, own, lands, picks, rate, start):
    columns = lands.shape[1]
    peers = owners.shape[0] * LANES // columns
    slots = lands.shape[0] // peers
    picks[...] = chosen_slots(me, owners, peers, slots)
    spans = rows_of(owners, peers)
    hits = spans // columns == me[0]
    order = earlier(hits, columns)
    local = (spans % columns + 1).astype(jnp.float32)
    spot_of = lax.broadcasted_iota(jnp.int32, (peers, columns), 1).astype(jnp.float32)
    for k in range(slots):
        spot = jnp.sum(jnp.where(hits & (order == k), local, 0.0), axis=1, keepdims=True)
        lands[k * peers : (k + 1) * peers, :] = jnp.where(spot - 1.0 == spot_of, 1.0, 0.0).astype(
            jnp.bfloat16
        )
    even = lax.broadcasted_iota(jnp.int32, (8, LANES), 0) % 2 == 0
    fraction = cond_rate * flags[...].astype(jnp.float32)
    first, second = (
        jnp.broadcast_to(fraction[:, c * LANES : (c + 1) * LANES], (8, LANES)) for c in (0, 1)
    )
    fraction = jnp.where(even, first, second)
    rate[0] = (latent_gain * GROWTH) * fraction
    rate[1] = fraction

    def body(z, carry):
        place(own, 0, start, z)
        return carry

    lax.fori_loop(0, own.shape[0] // 2, body, 0, unroll=2)


def forcing_kernel(got, lands, force, east, west, rows):
    columns = lands.shape[1]
    tiles = 9
    peers = got.shape[0] // tiles
    slots = lands.shape[0] // peers
    levels = east.shape[0]
    lane_tiles = rows.shape[0]
    half = LANES // 2
    landed = lands[...]
    stacked = jnp.concatenate(
        [got[pl.ds(k, peers, stride=tiles), :] for k in range(slots)], axis=0
    )
    forcing = sum(dot(piece, landed) for piece in thirds(stacked.T)) / STEPS
    wind = jnp.zeros((half, columns), jnp.float32)
    for j in range(slots // 2):
        turned = thirds(got[pl.ds(slots + j, peers, stride=tiles), :].T)
        for odd in range(2):
            where_to = landed[(2 * j + odd) * peers : (2 * j + odd + 1) * peers]
            for piece in turned:
                wind = wind + dot(piece[odd * half : (odd + 1) * half], where_to)
    for c in range(lane_tiles):
        lanes = slice(c * LANES, (c + 1) * LANES)
        rows[c, :LANES, :] = forcing[:, lanes]
        rows[c, LANES:, :] = 0.5 * wind[:, lanes]
    even = lax.broadcasted_iota(jnp.int32, (8, LANES), 0) % 2 == 0

    def woven(line):
        first, second = (jnp.broadcast_to(rows[c, pl.ds(line, 1), :], (8, LANES)) for c in (0, 1))
        return jnp.where(even, first, second)

    def weave(z, carry):
        force[z] = GROWTH * woven(z)
        force[levels + z] = woven(levels + z)
        along = woven(LANES + z)
        east[z] = diffuse_x - along
        west[z] = diffuse_x + along
        return carry

    lax.fori_loop(0, levels, weave, 0, unroll=2)


def place(slab, first, target, z):
    levels = target.shape[0] // 2
    for f in range(2):
        for c in range(2):
            value = slab[f * levels + z, 4 * c : 4 * c + 4, :]
            value = GROWTH * value - 1.0 if f == 0 else value + sat_scale
            target[f * levels + z, pl.ds(2 * first + c, 4, stride=2), :] = value


def march(force, east, west, rates, source, z, below, above, starts):
    levels = east.shape[0]
    results = []
    for row in starts:
        stepped = []
        for f in range(2):
            base = f * levels
            stepped.append(
                (1.0 - 2.0 * diffuse_x - 2.0 * diffuse_z) * source[base + z, row : row + 8, :]
                + diffuse_z
                * (source[base + below, row : row + 8, :] + source[base + above, row : row + 8, :])
                + (
                    east[z] * source[base + z, row + 2 : row + 10, :]
                    + west[z] * source[base + z, row - 2 : row + 6, :]
                )
                + force[base + z]
            )
        energy, moisture = stepped
        excess = jnp.maximum(moisture - jnp.exp2(energy), 0.0)
        results.append((energy + rates[0] * excess, moisture - rates[1] * excess))
    return results


def sweep(levels, many, work, keep):
    def body(i, carry):
        zs = [i * many + k for k in range(many)]
        found = [work(z, jnp.maximum(z - 1, 0), jnp.minimum(z + 1, levels - 1)) for z in zs]
        for z, results in zip(zs, found):
            keep(z, results)
        return carry

    lax.fori_loop(0, levels // many, body, 0)
    for z in range(levels // many * many, levels):
        keep(z, work(z, max(z - 1, 0), min(z + 1, levels - 1)))


NARROW = ((10, 18, 22), (12, 20), (14, 18), (16,))
MANY = (9, 29, 29, 29)


def inner_kernel(parity, force, east, west, rate, start, near0, near1, edges, even, odd):
    levels = east.shape[0]
    rates = (rate[0], rate[1])

    def fill(left, right):
        def body(z, carry):
            place(left, 4, even, z)
            place(right, 12, even, z)
            for i in (z, levels + z):
                even[i, 16:24, :] = start[i]
            return carry

        lax.fori_loop(0, levels, body, 0, unroll=2)

    @pl.when(parity[0] == 0)
    def _():
        fill(near1, near0)

    @pl.when(parity[0] == 1)
    def _():
        fill(near0, near1)

    def copy_edges(t, source):
        def body(i, carry):
            edges[t, i, 0:4, :] = source[i, 8 + 2 * t : 12 + 2 * t, :]
            edges[t, i, 4:8, :] = source[i, 28 - 2 * t : 32 - 2 * t, :]
            return carry

        lax.fori_loop(0, 2 * levels, body, 0, unroll=4)

    copy_edges(0, even)
    for t, starts in enumerate(NARROW):
        source, target = (even, odd) if t % 2 == 0 else (odd, even)

        def keep(z, results, target=target, starts=starts):
            for row, pair in zip(starts, results):
                for f, value in enumerate(pair):
                    target[f * levels + z, row : row + 8, :] = value

        def work(z, below, above, source=source, starts=starts):
            return march(force, east, west, rates, source, z, below, above, starts)

        sweep(levels, MANY[t], work, keep)
        copy_edges(t + 1, target)


def outer_side(left, far, force, east, west, rates, edges, even, odd):
    levels = east.shape[0]
    part = slice(0, 4) if left else slice(4, 8)

    def body(z, carry):
        place(far, 0 if left else 16, even, z)
        row = 8 if left else 28
        for i in (z, levels + z):
            even[i, row : row + 4, :] = edges[0, i, part, :]
        return carry

    lax.fori_loop(0, levels, body, 0, unroll=2)
    for t in range(4):
        source, target = (even, odd) if t % 2 == 0 else (odd, even)
        start = 2 * t + 2 if left else 30 - 2 * t
        row = 10 + 2 * t if left else 26 - 2 * t

        def keep(z, results, t=t, target=target, start=start, row=row):
            for f in range(2):
                i = f * levels + z
                target[i, start : start + 8, :] = results[0][f]
                target[i, row : row + 4, :] = edges[t + 1, i, part, :]

        def work(z, below, above, source=source, start=start):
            return march(force, east, west, rates, source, z, below, above, (start,))

        sweep(levels, 29, work, keep)


def side_kernel(parity, force, east, west, rate, far, edges, strip, even, odd):
    rates = (rate[0], rate[1])

    def run(left):
        outer_side(left, far, force, east, west, rates, edges, even, odd)
        row = 8 if left else 24

        def body(i, carry):
            strip[i] = even[i, row : row + 8, :]
            return carry

        lax.fori_loop(0, strip.shape[0], body, 0, unroll=4)

    pl.when(parity[0] == 0)(lambda: run(False))
    pl.when(parity[0] == 1)(lambda: run(True))


def outer_kernel(
    parity, force, east, west, rate, far, edges, strip, first, ended, change, even, odd, sums
):
    levels = east.shape[0]
    rates = (rate[0], rate[1])
    share = change.shape[1] // 2
    sums[...] = jnp.zeros_like(sums)

    def run(left):
        outer_side(left, far, force, east, west, rates, edges, even, odd)
        row = 24 if left else 8
        inward = 20 if left else 16
        part = slice(4, 8) if left else slice(0, 4)

        def body(i, carry):
            even[i, row : row + 8, :] = strip[i]
            even[i, inward : inward + 4, :] = edges[4, i, part, :]
            return carry

        lax.fori_loop(0, 2 * levels, body, 0, unroll=4)

    pl.when(parity[0] == 0)(lambda: run(True))
    pl.when(parity[0] == 1)(lambda: run(False))
    for t, starts in enumerate(NARROW):
        source, target = (even, odd) if t % 2 == 0 else (odd, even)

        def keep(z, results, t=t, target=target, starts=starts):
            for row, pair in zip(starts, results):
                for f, value in enumerate(pair):
                    i = f * levels + z
                    if t < len(NARROW) - 1:
                        target[i, row : row + 8, :] = value
                        continue
                    grown = value - first[i]
                    ended[i] = (value + 1.0) * (1.0 / GROWTH) if f == 0 else value - sat_scale
                    grown = grown + pltpu.roll(grown, 2, 0)
                    grown = grown + pltpu.roll(grown, 4, 0)
                    for c in range(2):
                        sums[f, c, pl.ds(z, 1), :] = grown[c : c + 1, :]

        def work(z, below, above, source=source, starts=starts):
            return march(force, east, west, rates, source, z, below, above, starts)

        sweep(levels, MANY[t], work, keep)

    for f in range(2):
        scale = 1.0 / GROWTH if f == 0 else 1.0
        for c in range(2):
            for g in range(change.shape[0]):
                change[g, f * share : (f + 1) * share, c * LANES : (c + 1) * LANES] = (
                    scale * sums[f, c, g * share : (g + 1) * share, :]
                )


def finish_kernel(ended, final):
    def body(i, carry):
        for c in range(2):
            final[i, 4 * c : 4 * c + 4, :] = ended[i, pl.ds(c, 4, stride=2), :]
        return carry

    lax.fori_loop(0, final.shape[0], body, 0, unroll=4)


def return_kernel(inverse, parts, lands, sent):
    pieces, rows, columns = parts.shape
    peers = sent.shape[0]
    slots = lands.shape[0] // peers
    total = parts[0]
    for g in range(1, pieces):
        total = total + parts[g]
    total = total * inverse[0]
    many = jnp.concatenate([total] * (LANES // rows), axis=0)
    placed = sum(dot(lands[...], piece, ((1,), (1,))) for piece in thirds(many))
    lane = lax.broadcasted_iota(jnp.int32, (peers, LANES), 1) // rows
    out = jnp.zeros((peers, LANES), jnp.float32)
    for k in range(slots):
        out = out + jnp.where(lane == k, placed[k * peers : (k + 1) * peers], 0.0)
    sent[...] = out


def arrive_kernel(got, picks, copies):
    peers = got.shape[0]
    slots = picks.shape[0] // peers
    pieces, rows, columns = copies.shape
    turned = thirds(got[...].T)
    share = jnp.zeros((rows, columns), jnp.float32)
    for k in range(slots):
        where_to = picks[k * peers : (k + 1) * peers]
        for piece in turned:
            share = share + dot(piece, where_to)[k * rows : (k + 1) * rows]
    for g in range(pieces):
        copies[g] = share


def spread_kernel(every, tendency):
    pieces, rows, columns = every.shape
    share = rows // 2
    levels = tendency.shape[0] // 2
    for f in range(2):
        for g in range(pieces):
            here = min(share, levels - g * share)
            if here > 0:
                start = f * levels + g * share
                tendency[start : start + here, :] = every[g, f * share : f * share + here, :]


def call(kernel, outs, scratch=(), scalars=0, inputs=0, limit=16):
    return pl.pallas_call(
        kernel,
        out_shape=outs,
        in_specs=[SMEM] * scalars + [VMEM] * inputs,
        out_specs=jax.tree.map(lambda _: VMEM, outs),
        scratch_shapes=list(scratch),
        compiler_params=pltpu.CompilerParams(vmem_limit_bytes=limit * 1024 * 1024),
    )


def swapped(x, odd):
    peers = lax.axis_size("grp")
    return lax.ppermute(
        x, "grp", [(i, (i + 1 if i % 2 == odd else i - 1) % peers) for i in range(peers)]
    )


def traded(x, axis):
    return lax.all_to_all(x, axis, split_axis=0, concat_axis=0, tiled=True)


def flat(x):
    f, z, cells, columns = x.shape
    x = x.reshape(f, z, cells, columns // LANES, LANES).transpose(0, 1, 3, 2, 4)
    return x.reshape(f * z, cells * columns // LANES, LANES)


def on_device(profiles, courant, owner_map, cloud_flags, crm_state):
    columns, feats = profiles.shape
    levels = courant.shape[1]
    col_count = lax.axis_size("col")
    pieces = lax.axis_size("grp")
    fields, _, cells, _ = crm_state.shape
    per_peer = columns // col_count
    capacity = per_peer + min(2, per_peer)
    share = -(-levels // pieces)
    tall = share * pieces
    lane_tiles = columns // LANES
    f32, bf16 = jnp.float32, jnp.bfloat16
    S = jax.ShapeDtypeStruct
    me = lax.axis_index("col").reshape(1)
    owners = owner_map.reshape(-1, LANES)
    near0, near1 = swapped(crm_state, 0), swapped(crm_state, 1)
    tiles = capacity + capacity // 2
    packed = call(pack_kernel, S((col_count * tiles, LANES), f32), (), 1, 3, 60)(
        me, owners, profiles.T, courant.T
    )
    got = traded(packed.reshape(col_count, 1, tiles * LANES), "col").reshape(packed.shape)
    chosen = S((capacity * col_count, columns), bf16)
    lines = fields * levels
    lands, picks, rate, start = call(
        landing_kernel,
        (chosen, chosen, S((2, 8, LANES), f32), S((lines, 8, LANES), f32)),
        (),
        1,
        3,
    )(me, owners, cloud_flags.reshape(1, columns), flat(crm_state))
    far0, far1 = swapped(near1, 0), swapped(near0, 1)
    forces = call(
        forcing_kernel,
        (
            S((lines, 8, LANES), f32),
            S((levels, 8, LANES), f32),
            S((levels, 8, LANES), f32),
        ),
        [pltpu.VMEM((lane_tiles, 3 * LANES // 2, LANES), f32)],
        0,
        2,
    )(got, lands)
    parity = (lax.axis_index("grp") % 2).reshape(1)
    state = pltpu.VMEM((lines, 40, LANES), f32)
    edges = call(inner_kernel, S((5, lines, 8, LANES), f32), [state, state], 1, 7)(
        parity, *forces, rate, start, flat(near0), flat(near1)
    )
    strip = call(side_kernel, S((lines, 8, LANES), f32), [state, state], 1, 6)(
        parity, *forces, rate, flat(far0), edges
    )
    ended, change = call(
        outer_kernel,
        (S((lines, 8, LANES), f32), S((pieces, 2 * share, columns), f32)),
        [state, state, pltpu.VMEM((fields, lane_tiles, tall, LANES), f32)],
        1,
        8,
    )(parity, *forces, rate, flat(far1), edges, strip, start)
    rows = call(finish_kernel, S((lines, 8, LANES), f32), (), 0, 1)(ended)
    rows = rows.reshape(fields, levels, lane_tiles, cells, LANES).transpose(0, 1, 3, 2, 4)
    crm_final = rows.reshape(crm_state.shape)
    parts = traded(change, "grp")
    inverse = jnp.full((1,), 1.0 / (pieces * cells), f32)
    back = call(return_kernel, S((col_count, LANES), f32), (), 1, 2)(inverse, parts, lands)
    back = traded(back.reshape(col_count, 1, LANES), "col").reshape(back.shape)
    copies = call(arrive_kernel, S((pieces, 2 * share, columns), f32), (), 0, 2)(back, picks)
    every = traded(copies, "grp")
    tendency = call(spread_kernel, S((feats, columns), f32), (), 0, 1)(every)
    return tendency.T, crm_final


def solution(mesh):
    placed = (P("col", None), P("col", None), P(), P("col"), P(None, None, "grp", "col"))
    return jax.shard_map(
        on_device,
        mesh=mesh,
        in_specs=placed,
        out_specs=(P("col", None), P(None, None, "grp", "col")),
        check_vma=False,
    )
```

```python
import functools

import jax
import jax.numpy as jnp
from jax import lax
from jax.experimental import pallas as pl
from jax.experimental.pallas import tpu as pltpu
from jax.sharding import PartitionSpec as P

STEPS = 8

diffuse_x = 0.25
diffuse_z = 0.2
sat_scale = 0.5
sat_slope = 0.3
cond_rate = 0.5
latent_gain = 0.4

LANES = 128
GROWTH = sat_slope * 1.4426950408889634
VMEM = pl.BlockSpec(memory_space=pltpu.VMEM)
SMEM = pl.BlockSpec(memory_space=pltpu.SMEM)


def thirds(x):
    first = x.astype(jnp.bfloat16)
    rest = x - first.astype(jnp.float32)
    second = rest.astype(jnp.bfloat16)
    third = (rest - second.astype(jnp.float32)).astype(jnp.bfloat16)
    return first, second, third


def dot(a, b, dims=((1,), (0,))):
    return lax.dot_general(a, b, (dims, ((), ())), preferred_element_type=jnp.float32)


def earlier(hits, count):
    row = lax.broadcasted_iota(jnp.int32, (count, count), 0)
    col = lax.broadcasted_iota(jnp.int32, (count, count), 1)
    strict = jnp.where(row < col, 1.0, 0.0).astype(jnp.bfloat16)
    return dot(jnp.where(hits, 1.0, 0.0).astype(jnp.bfloat16), strict)


def rows_of(owners, count):
    left = owners[pl.ds(0, count, stride=2), :]
    right = owners[pl.ds(1, count, stride=2), :]
    return jnp.concatenate([left, right], axis=1)


def chosen_slots(me, owners, peers, slots):
    mine = [owners[pl.ds(2 * me[0] + i, 1), :] for i in range(2)]
    mine = jnp.concatenate(mine, axis=1)
    columns = mine.shape[1]
    hits = lax.broadcasted_iota(jnp.int32, (peers, columns), 0) == mine // columns
    order = earlier(hits, columns)
    return jnp.concatenate(
        [jnp.where(hits & (order == k), 1.0, 0.0) for k in range(slots)], axis=0
    ).astype(jnp.bfloat16)


def pack_kernel(me, owners, prof, cour, packed):
    feats, columns = prof.shape
    levels = cour.shape[0]
    peers = owners.shape[0] * LANES // columns
    tiles = packed.shape[0] // peers
    slots = tiles * 2 // 3
    half = LANES // 2
    chosen = chosen_slots(me, owners, peers, slots)
    gap = jnp.zeros((half - levels, columns), jnp.float32)
    wind = jnp.concatenate([cour[...], gap], axis=0)
    table = jnp.concatenate(
        [prof[...], jnp.zeros((LANES - feats, columns), jnp.float32), wind, wind], axis=0
    )
    rows = sum(dot(chosen, piece, ((1,), (1,))) for piece in thirds(table))
    for k in range(slots):
        packed[pl.ds(k, peers, stride=tiles), :] = rows[k * peers : (k + 1) * peers, :LANES]
    first_half = lax.broadcasted_iota(jnp.int32, (peers, LANES), 1) < half
    for j in range(slots // 2):
        low = rows[2 * j * peers : (2 * j + 1) * peers, LANES : 2 * LANES]
        high = rows[(2 * j + 1) * peers : (2 * j + 2) * peers, LANES : 2 * LANES]
        packed[pl.ds(slots + j, peers, stride=tiles), :] = jnp.where(first_half, low, high)


def landing_kernel(me, owners, flags, own, lands, picks, rate, start):
    columns = lands.shape[1]
    peers = owners.shape[0] * LANES // columns
    slots = lands.shape[0] // peers
    picks[...] = chosen_slots(me, owners, peers, slots)
    spans = rows_of(owners, peers)
    hits = spans // columns == me[0]
    order = earlier(hits, columns)
    local = (spans % columns + 1).astype(jnp.float32)
    spot_of = lax.broadcasted_iota(jnp.int32, (peers, columns), 1).astype(jnp.float32)
    for k in range(slots):
        spot = jnp.sum(jnp.where(hits & (order == k), local, 0.0), axis=1, keepdims=True)
        lands[k * peers : (k + 1) * peers, :] = jnp.where(spot - 1.0 == spot_of, 1.0, 0.0).astype(
            jnp.bfloat16
        )
    even = lax.broadcasted_iota(jnp.int32, (8, LANES), 0) % 2 == 0
    fraction = cond_rate * flags[...].astype(jnp.float32)
    first, second = (
        jnp.broadcast_to(fraction[:, c * LANES : (c + 1) * LANES], (8, LANES)) for c in (0, 1)
    )
    fraction = jnp.where(even, first, second)
    rate[0] = (latent_gain * GROWTH) * fraction
    rate[1] = fraction

    def body(z, carry):
        place(own, 0, start, z)
        return carry

    lax.fori_loop(0, own.shape[0] // 2, body, 0, unroll=2)


def forcing_kernel(got, lands, force, east, west, rows):
    columns = lands.shape[1]
    tiles = 9
    peers = got.shape[0] // tiles
    slots = lands.shape[0] // peers
    levels = east.shape[0]
    lane_tiles = rows.shape[0]
    half = LANES // 2
    landed = lands[...]
    stacked = jnp.concatenate(
        [got[pl.ds(k, peers, stride=tiles), :] for k in range(slots)], axis=0
    )
    forcing = sum(dot(piece, landed) for piece in thirds(stacked.T)) / STEPS
    wind = jnp.zeros((half, columns), jnp.float32)
    for j in range(slots // 2):
        turned = thirds(got[pl.ds(slots + j, peers, stride=tiles), :].T)
        for odd in range(2):
            where_to = landed[(2 * j + odd) * peers : (2 * j + odd + 1) * peers]
            for piece in turned:
                wind = wind + dot(piece[odd * half : (odd + 1) * half], where_to)
    for c in range(lane_tiles):
        lanes = slice(c * LANES, (c + 1) * LANES)
        rows[c, :LANES, :] = forcing[:, lanes]
        rows[c, LANES:, :] = 0.5 * wind[:, lanes]
    even = lax.broadcasted_iota(jnp.int32, (8, LANES), 0) % 2 == 0

    def woven(line):
        first, second = (jnp.broadcast_to(rows[c, pl.ds(line, 1), :], (8, LANES)) for c in (0, 1))
        return jnp.where(even, first, second)

    def weave(z, carry):
        force[z] = GROWTH * woven(z)
        force[levels + z] = woven(levels + z)
        along = woven(LANES + z)
        east[z] = diffuse_x - along
        west[z] = diffuse_x + along
        return carry

    lax.fori_loop(0, levels, weave, 0, unroll=2)


def place(slab, first, target, z):
    levels = target.shape[0] // 2
    for f in range(2):
        for c in range(2):
            value = slab[f * levels + z, 4 * c : 4 * c + 4, :]
            value = GROWTH * value - 1.0 if f == 0 else value + sat_scale
            target[f * levels + z, pl.ds(2 * first + c, 4, stride=2), :] = value


def march(force, east, west, rates, source, z, below, above, starts):
    levels = east.shape[0]
    results = []
    for row in starts:
        stepped = []
        for f in range(2):
            base = f * levels
            stepped.append(
                (1.0 - 2.0 * diffuse_x - 2.0 * diffuse_z) * source[base + z, row : row + 8, :]
                + diffuse_z
                * (source[base + below, row : row + 8, :] + source[base + above, row : row + 8, :])
                + (
                    east[z] * source[base + z, row + 2 : row + 10, :]
                    + west[z] * source[base + z, row - 2 : row + 6, :]
                )
                + force[base + z]
            )
        energy, moisture = stepped
        excess = jnp.maximum(moisture - jnp.exp2(energy), 0.0)
        results.append((energy + rates[0] * excess, moisture - rates[1] * excess))
    return results


def sweep(levels, many, work, keep):
    def body(i, carry):
        zs = [i * many + k for k in range(many)]
        found = [work(z, jnp.maximum(z - 1, 0), jnp.minimum(z + 1, levels - 1)) for z in zs]
        for z, results in zip(zs, found):
            keep(z, results)
        return carry

    lax.fori_loop(0, levels // many, body, 0)
    for z in range(levels // many * many, levels):
        keep(z, work(z, max(z - 1, 0), min(z + 1, levels - 1)))


NARROW = ((10, 18, 22), (12, 20), (14, 18), (16,))
MANY = (9, 29, 29, 29)


def inner_kernel(parity, force, east, west, rate, start, near0, near1, edges, even, odd):
    levels = east.shape[0]
    rates = (rate[0], rate[1])

    def fill(left, right):
        def body(z, carry):
            place(left, 4, even, z)
            place(right, 12, even, z)
            for i in (z, levels + z):
                even[i, 16:24, :] = start[i]
            return carry

        lax.fori_loop(0, levels, body, 0, unroll=2)

    @pl.when(parity[0] == 0)
    def _():
        fill(near1, near0)

    @pl.when(parity[0] == 1)
    def _():
        fill(near0, near1)

    def copy_edges(t, source):
        def body(i, carry):
            edges[t, i, 0:4, :] = source[i, 8 + 2 * t : 12 + 2 * t, :]
            edges[t, i, 4:8, :] = source[i, 28 - 2 * t : 32 - 2 * t, :]
            return carry

        lax.fori_loop(0, 2 * levels, body, 0, unroll=4)

    copy_edges(0, even)
    for t, starts in enumerate(NARROW):
        source, target = (even, odd) if t % 2 == 0 else (odd, even)

        def keep(z, results, target=target, starts=starts):
            for row, pair in zip(starts, results):
                for f, value in enumerate(pair):
                    target[f * levels + z, row : row + 8, :] = value

        def work(z, below, above, source=source, starts=starts):
            return march(force, east, west, rates, source, z, below, above, starts)

        sweep(levels, MANY[t], work, keep)
        copy_edges(t + 1, target)


def outer_side(left, far, force, east, west, rates, edges, even, odd):
    levels = east.shape[0]
    part = slice(0, 4) if left else slice(4, 8)

    def body(z, carry):
        place(far, 0 if left else 16, even, z)
        row = 8 if left else 28
        for i in (z, levels + z):
            even[i, row : row + 4, :] = edges[0, i, part, :]
        return carry

    lax.fori_loop(0, levels, body, 0, unroll=2)
    for t in range(4):
        source, target = (even, odd) if t % 2 == 0 else (odd, even)
        start = 2 * t + 2 if left else 30 - 2 * t
        row = 10 + 2 * t if left else 26 - 2 * t

        def keep(z, results, t=t, target=target, start=start, row=row):
            for f in range(2):
                i = f * levels + z
                target[i, start : start + 8, :] = results[0][f]
                target[i, row : row + 4, :] = edges[t + 1, i, part, :]

        def work(z, below, above, source=source, start=start):
            return march(force, east, west, rates, source, z, below, above, (start,))

        sweep(levels, 29, work, keep)


def side_kernel(parity, force, east, west, rate, far, edges, strip, even, odd):
    rates = (rate[0], rate[1])

    def run(left):
        outer_side(left, far, force, east, west, rates, edges, even, odd)
        row = 8 if left else 24

        def body(i, carry):
            strip[i] = even[i, row : row + 8, :]
            return carry

        lax.fori_loop(0, strip.shape[0], body, 0, unroll=4)

    pl.when(parity[0] == 0)(lambda: run(False))
    pl.when(parity[0] == 1)(lambda: run(True))


def outer_kernel(
    parity, force, east, west, rate, far, edges, strip, first, ended, change, even, odd, sums
):
    levels = east.shape[0]
    rates = (rate[0], rate[1])
    share = change.shape[1] // 2
    sums[...] = jnp.zeros_like(sums)

    def run(left):
        outer_side(left, far, force, east, west, rates, edges, even, odd)
        row = 24 if left else 8
        inward = 20 if left else 16
        part = slice(4, 8) if left else slice(0, 4)

        def body(i, carry):
            even[i, row : row + 8, :] = strip[i]
            even[i, inward : inward + 4, :] = edges[4, i, part, :]
            return carry

        lax.fori_loop(0, 2 * levels, body, 0, unroll=4)

    pl.when(parity[0] == 0)(lambda: run(True))
    pl.when(parity[0] == 1)(lambda: run(False))
    for t, starts in enumerate(NARROW):
        source, target = (even, odd) if t % 2 == 0 else (odd, even)

        def keep(z, results, t=t, target=target, starts=starts):
            for row, pair in zip(starts, results):
                for f, value in enumerate(pair):
                    i = f * levels + z
                    if t < len(NARROW) - 1:
                        target[i, row : row + 8, :] = value
                        continue
                    grown = value - first[i]
                    ended[i] = (value + 1.0) * (1.0 / GROWTH) if f == 0 else value - sat_scale
                    grown = grown + pltpu.roll(grown, 2, 0)
                    grown = grown + pltpu.roll(grown, 4, 0)
                    for c in range(2):
                        sums[f, c, pl.ds(z, 1), :] = grown[c : c + 1, :]

        def work(z, below, above, source=source, starts=starts):
            return march(force, east, west, rates, source, z, below, above, starts)

        sweep(levels, MANY[t], work, keep)

    for f in range(2):
        scale = 1.0 / GROWTH if f == 0 else 1.0
        for c in range(2):
            for g in range(change.shape[0]):
                change[g, f * share : (f + 1) * share, c * LANES : (c + 1) * LANES] = (
                    scale * sums[f, c, g * share : (g + 1) * share, :]
                )


def finish_kernel(ended, final):
    def body(i, carry):
        for c in range(2):
            final[i, 4 * c : 4 * c + 4, :] = ended[i, pl.ds(c, 4, stride=2), :]
        return carry

    lax.fori_loop(0, final.shape[0], body, 0, unroll=4)


def return_kernel(inverse, parts, lands, sent):
    pieces, rows, columns = parts.shape
    peers = sent.shape[0]
    slots = lands.shape[0] // peers
    total = parts[0]
    for g in range(1, pieces):
        total = total + parts[g]
    total = total * inverse[0]
    many = jnp.concatenate([total] * (LANES // rows), axis=0)
    placed = sum(dot(lands[...], piece, ((1,), (1,))) for piece in thirds(many))
    lane = lax.broadcasted_iota(jnp.int32, (peers, LANES), 1) // rows
    out = jnp.zeros((peers, LANES), jnp.float32)
    for k in range(slots):
        out = out + jnp.where(lane == k, placed[k * peers : (k + 1) * peers], 0.0)
    sent[...] = out


def arrive_kernel(got, picks, copies):
    peers = got.shape[0]
    slots = picks.shape[0] // peers
    pieces, rows, columns = copies.shape
    turned = thirds(got[...].T)
    share = jnp.zeros((rows, columns), jnp.float32)
    for k in range(slots):
        where_to = picks[k * peers : (k + 1) * peers]
        for piece in turned:
            share = share + dot(piece, where_to)[k * rows : (k + 1) * rows]
    for g in range(pieces):
        copies[g] = share


def spread_kernel(every, tendency):
    pieces, rows, columns = every.shape
    share = rows // 2
    levels = tendency.shape[0] // 2
    for f in range(2):
        for g in range(pieces):
            here = min(share, levels - g * share)
            if here > 0:
                start = f * levels + g * share
                tendency[start : start + here, :] = every[g, f * share : f * share + here, :]


def call(kernel, outs, scratch=(), scalars=0, inputs=0, limit=16):
    return pl.pallas_call(
        kernel,
        out_shape=outs,
        in_specs=[SMEM] * scalars + [VMEM] * inputs,
        out_specs=jax.tree.map(lambda _: VMEM, outs),
        scratch_shapes=list(scratch),
        compiler_params=pltpu.CompilerParams(vmem_limit_bytes=limit * 1024 * 1024),
    )


def swapped(x, odd):
    peers = lax.axis_size("grp")
    return lax.ppermute(
        x, "grp", [(i, (i + 1 if i % 2 == odd else i - 1) % peers) for i in range(peers)]
    )


def traded(x, axis):
    return lax.all_to_all(x, axis, split_axis=0, concat_axis=0, tiled=True)


def flat(x):
    f, z, cells, columns = x.shape
    x = x.reshape(f, z, cells, columns // LANES, LANES).transpose(0, 1, 3, 2, 4)
    return x.reshape(f * z, cells * columns // LANES, LANES)


def on_device(profiles, courant, owner_map, cloud_flags, crm_state):
    columns, feats = profiles.shape
    levels = courant.shape[1]
    col_count = lax.axis_size("col")
    pieces = lax.axis_size("grp")
    fields, _, cells, _ = crm_state.shape
    per_peer = columns // col_count
    capacity = per_peer + min(2, per_peer)
    share = -(-levels // pieces)
    tall = share * pieces
    lane_tiles = columns // LANES
    f32, bf16 = jnp.float32, jnp.bfloat16
    S = jax.ShapeDtypeStruct
    me = lax.axis_index("col").reshape(1)
    owners = owner_map.reshape(-1, LANES)
    near0, near1 = swapped(crm_state, 0), swapped(crm_state, 1)
    tiles = capacity + capacity // 2
    packed = call(pack_kernel, S((col_count * tiles, LANES), f32), (), 1, 3, 60)(
        me, owners, profiles.T, courant.T
    )
    got = traded(packed.reshape(col_count, 1, tiles * LANES), "col").reshape(packed.shape)
    chosen = S((capacity * col_count, columns), bf16)
    lines = fields * levels
    lands, picks, rate, start = call(
        landing_kernel,
        (chosen, chosen, S((2, 8, LANES), f32), S((lines, 8, LANES), f32)),
        (),
        1,
        3,
    )(me, owners, cloud_flags.reshape(1, columns), flat(crm_state))
    far0, far1 = swapped(near1, 0), swapped(near0, 1)
    forces = call(
        forcing_kernel,
        (
            S((lines, 8, LANES), f32),
            S((levels, 8, LANES), f32),
            S((levels, 8, LANES), f32),
        ),
        [pltpu.VMEM((lane_tiles, 3 * LANES // 2, LANES), f32)],
        0,
        2,
    )(got, lands)
    parity = (lax.axis_index("grp") % 2).reshape(1)
    state = pltpu.VMEM((lines, 40, LANES), f32)
    edges = call(inner_kernel, S((5, lines, 8, LANES), f32), [state, state], 1, 7)(
        parity, *forces, rate, start, flat(near0), flat(near1)
    )
    strip = call(side_kernel, S((lines, 8, LANES), f32), [state, state], 1, 6)(
        parity, *forces, rate, flat(far0), edges
    )
    ended, change = call(
        outer_kernel,
        (S((lines, 8, LANES), f32), S((pieces, 2 * share, columns), f32)),
        [state, state, pltpu.VMEM((fields, lane_tiles, tall, LANES), f32)],
        1,
        8,
    )(parity, *forces, rate, flat(far1), edges, strip, start)
    rows = call(finish_kernel, S((lines, 8, LANES), f32), (), 0, 1)(ended)
    rows = rows.reshape(fields, levels, lane_tiles, cells, LANES).transpose(0, 1, 3, 2, 4)
    crm_final = rows.reshape(crm_state.shape)
    parts = traded(change, "grp")
    inverse = jnp.full((1,), 1.0 / (pieces * cells), f32)
    back = call(return_kernel, S((col_count, LANES), f32), (), 1, 2)(inverse, parts, lands)
    back = traded(back.reshape(col_count, 1, LANES), "col").reshape(back.shape)
    copies = call(arrive_kernel, S((pieces, 2 * share, columns), f32), (), 0, 2)(back, picks)
    every = traded(copies, "grp")
    tendency = call(spread_kernel, S((feats, columns), f32), (), 0, 1)(every)
    return tendency.T, crm_final


def solution(mesh):
    placed = (P("col", None), P("col", None), P(), P("col"), P(None, None, "grp", "col"))
    return jax.shard_map(
        on_device,
        mesh=mesh,
        in_specs=placed,
        out_specs=(P("col", None), P(None, None, "grp", "col")),
        check_vma=False,
    )
```
